32 devices in a mesh: owner: 4 (over z), rows: 8 (over y, x, core).
Axes of the slice: x: 2, y: 2, z: 4, core: 2. Of those that a mesh axis runs over, the one named last changes fastest.
Arguments:
- w_gate: float32 [128, 2048, 768], P('owner', 'rows'), may hold values from -0.1875 to 0.1875
- w_up: float32 [128, 2048, 768], P('owner', 'rows'), may hold values from -0.1875 to 0.1875
- router_weight: float32 [2048, 128], P('rows', 'owner'), may hold values from -0.125 to 0.125
- router_gain: float32 [2048], P('rows'), may hold values from 0.25 to 1.75
Outputs:
- serve_gate: bfloat16 [128, 2048, 768], P('owner', None, 'rows')
- serve_up: bfloat16 [128, 2048, 768], P('owner', None, 'rows')
- scale_gate: float32 [128, 768], P('owner', 'rows')
- scale_up: float32 [128, 768], P('owner', 'rows')
- serve_router: bfloat16 [2048, 128], replicated
The draws below stay inside these ranges and needn't reach their ends.
All inputs are finite; a program needn't handle non-finite values. Where the reference program divides by a largest or mean magnitude, that divisor is 1e-20 or more.
Results may differ from the reference program's by a relative error of at most 0.001.
Values may be sent and summed in bfloat16 or wider, within the bound.
A program may use at most 192 MiB of HBM per device.

```python
import jax
import jax.numpy as jnp

EXPERTS = 128
D_MODEL = 2048
D_EXPERT = 768


def spiked(result, key, source, target, blocks, factor):
    owner, partner = [(jnp.arange(result.shape[dim]) // (result.shape[dim] // blocks)).reshape([-1 if axis == dim else 1 for axis in range(result.ndim)]) for dim in (source, target)]
    chosen = jax.random.permutation(key, blocks)[partner]
    strong = (owner == chosen) | (owner == (partner + blocks // 2) % blocks)
    return jnp.where(strong, factor * result, result)


def shard_levels(stream_key, extent, cuts, least, high):
    factor_of = 1.0
    for axis_at, parts in cuts:
        draws = jax.random.uniform(jax.random.fold_in(jax.random.fold_in(stream_key, 6), axis_at), (parts,), jnp.float32, least / len(cuts), high / len(cuts))
        factor_of = factor_of * jnp.repeat(jnp.exp(draws), extent[axis_at] // parts).reshape((-1,) + (1,) * (len(extent) - 1 - axis_at))
    return factor_of


def bell_draw(key, extent, spread, reach, cuts=(), held_as=jnp.bfloat16):
    loudness = shard_levels(key, extent, cuts, -0.22, 0.18) if cuts else 1.0
    entries = jax.random.normal(key, extent, jnp.float32) * spread * loudness
    return jnp.minimum(jnp.maximum(entries, -reach), reach).astype(held_as)


def bell_draw_with(key, dims, deviation, most, pieces, heavy, held_as=jnp.bfloat16):
    drawn = deviation * jax.random.normal(key, dims, jnp.float32)
    if pieces:
        drawn = drawn * shard_levels(key, dims, pieces, -0.22, 0.18)
    return jnp.clip(spiked(drawn, jax.random.fold_in(key, 3), *heavy), -most, most).astype(held_as)


def setup_inputs(seed: int = 0) -> dict:
    keys = jax.random.split(jax.random.key(seed), 5)
    w_gate = bell_draw_with(keys[0], (EXPERTS, D_MODEL, D_EXPERT), D_MODEL ** -0.5, 0.1875, ((0, 4), (1, 8)), (1, 2, 8, 2.0), jnp.float32)
    w_up = bell_draw_with(keys[1], (EXPERTS, D_MODEL, D_EXPERT), D_MODEL ** -0.5, 0.1875, ((0, 4), (1, 8)), (1, 2, 8, 2.0), jnp.float32)
    router_weight = bell_draw(keys[2], (D_MODEL, EXPERTS), D_MODEL ** -0.5, 0.125, ((0, 8), (1, 4)), jnp.float32)
    router_gain = jnp.clip(1.0 + 0.15 * jax.random.normal(keys[3], (D_MODEL,), jnp.float32), 0.25, 1.75)
    return {"w_gate": w_gate, "w_up": w_up, "router_weight": router_weight, "router_gain": router_gain}


def reference(w_gate, w_up, router_weight, router_gain):
    scale_gate = jnp.sum(jnp.abs(w_gate), axis=1) / D_MODEL
    serve_gate = (w_gate / jnp.expand_dims(scale_gate, 1)).astype(jnp.bfloat16)
    scale_up = jnp.sum(jnp.abs(w_up), axis=1) / D_MODEL
    serve_up = (w_up / jnp.expand_dims(scale_up, 1)).astype(jnp.bfloat16)
    serve_router = (router_weight * router_gain[:, None]).astype(jnp.bfloat16)
    return serve_gate, serve_up, scale_gate, scale_up, serve_router
```

```python
import functools

import jax
import jax.numpy as jnp
from jax import lax
from jax.experimental import pallas as pl
from jax.experimental.pallas import tpu as pltpu
from jax.sharding import PartitionSpec as P

MESH = pl.DeviceIdType.MESH
WINDOW = 3
LOADS = 3
LEAD = 8
X_LAG, Y_LAG, HALF_LAG = 1, 4, 7
HELD = LOADS + LEAD
SUMS = 2 * LEAD + 2
WRITES = 4


def peer_steps(n):
    far = list(range(2, n, 2))
    return far + [k + 1 for k in far] + [1]


def toggled(index, k):
    result, bit = index, 1
    while bit <= k:
        if k & bit:
            result = result + bit * (1 - 2 * lax.rem(index // bit, 2))
        bit *= 2
    return result


def exchange(
    experts, n, owners, depth, steps,
    gate, up, router, gain,
    pieces, routed, scales,
    window, stage, weight, gains, part, early, partner, chip, others, whole,
    load_sem, send_sem, recv_sem, pair_send, pair_recv, sum_send, sum_recv, last_send, last_recv,
    early_send, early_recv, in_sem, r_send, r_recv, z_send, z_recv, c_send, c_recv,
):
    me, mine = lax.axis_index("rows"), lax.axis_index("owner")
    units, piece, rows, width = 2 * experts, pieces.shape[1], gate.shape[1], gate.shape[2]
    lead = early.shape[1]
    peers = [toggled(me, k) for k in peer_steps(n)]
    alike = [toggled(me, k) for k in range(2, n, 2)]
    core, beside = lax.rem(me, 2), toggled(me, 1)
    columns = [lax.rem(mine + k, owners) for k in range(1, owners)]

    barrier = pltpu.get_barrier_semaphore()
    for p in peers:
        pl.semaphore_signal(barrier, inc=1, device_id=(mine, p), device_id_type=MESH)
    for c in columns:
        pl.semaphore_signal(barrier, inc=1, device_id=(c, me), device_id_type=MESH)

    def load(s, go):
        for matrix, first in ((gate, 0), (up, experts)):
            @pl.when((s >= first) & (s < first + experts))
            def _():
                slot = lax.rem(s, HELD)
                copy = pltpu.make_async_copy(matrix.at[s - first], window.at[slot], load_sem.at[slot])
                copy.start() if go else copy.wait()

    def pair(s):
        slot = lax.rem(s, SUMS)
        return pltpu.make_async_remote_copy(
            part.at[s, 1 - core], partner.at[s], pair_send.at[slot], pair_recv.at[slot],
            device_id=(mine, beside), device_id_type=MESH,
        )

    def chips(s, t):
        slot = lax.rem(s, SUMS)
        return pltpu.make_async_remote_copy(
            chip.at[s, t], others.at[s, t], sum_send.at[slot, t], sum_recv.at[slot, t],
            device_id=(mine, toggled(me, steps[t])), device_id_type=MESH,
        )

    def halves(s):
        slot = lax.rem(s, SUMS)
        return pltpu.make_async_remote_copy(
            whole.at[s, core], whole.at[s, core], last_send.at[slot], last_recv.at[slot],
            device_id=(mine, beside), device_id_type=MESH,
        )

    def direct(g):
        first, count = ((0, 1), (1, lead - 1))[g]
        return [
            pltpu.make_async_remote_copy(
                part.at[pl.ds(first, count)], early.at[me, pl.ds(first, count)],
                early_send.at[g, i], early_recv.at[g, i],
                device_id=(mine, p), device_id_type=MESH,
            )
            for i, p in enumerate(peers)
        ]

    def far(s):
        slot, land = lax.rem(s, WINDOW), lax.rem(s, 2 * WINDOW)
        return [
            pltpu.make_async_remote_copy(
                stage.at[slot, pl.ds(pl.multiple_of(p * piece, piece), piece)],
                pieces.at[s, :, pl.ds(pl.multiple_of(me * rows, rows), rows)],
                send_sem.at[slot, i], recv_sem.at[land, i],
                device_id=(mine, p), device_id_type=MESH,
            )
            for i, p in enumerate(peers)
        ]

    def start(copies):
        for copy in copies:
            copy.start()

    def finish(copies):
        for copy in copies:
            copy.wait()

    def summed(s):
        half = width // 2
        for h in range(2):
            w = window[lax.rem(s, HELD), :, h * half : (h + 1) * half]
            part[s, h] = jnp.sum(jnp.abs(w), axis=0, keepdims=True)

    def early_total(first, last):
        for h in range(2):
            total = jnp.zeros((last - first, 1, width // 2), jnp.float32)
            for p in range(n):
                total = total + jnp.where(p == me, part[first:last, h], early[p, first:last, h])
            whole[first:last, h] = total

    def scaled(s):
        slot, held = lax.rem(s, WINDOW), lax.rem(s, HELD)
        scale = jnp.concatenate([whole[s, 0], whole[s, 1]], axis=1) / depth
        scales[s] = scale
        inverse = 1.0 / scale
        for at in range(0, width, 128):
            w = window[held, :, at : at + 128] * inverse[:, at : at + 128]
            stage[slot, at : at + 128, :] = w.T.astype(jnp.bfloat16)
        own = stage[slot, pl.ds(pl.multiple_of(me * piece, piece), piece), :]
        pieces[s, :, pl.ds(pl.multiple_of(me * rows, rows), rows)] = own

    fetch = [
        pltpu.make_async_copy(router, weight, in_sem.at[0]),
        pltpu.make_async_copy(gain, gains, in_sem.at[1]),
    ]
    along_rows = [
        pltpu.make_async_remote_copy(
            routed.at[me, mine], routed.at[me, mine], r_send.at[i], r_recv.at[i],
            device_id=(mine, p), device_id_type=MESH,
        )
        for i, p in enumerate(alike)
    ]
    along_z = [
        pltpu.make_async_remote_copy(
            routed.at[p, mine], routed.at[p, mine], z_send.at[i, j], z_recv.at[i, j],
            device_id=(c, me), device_id_type=MESH,
        )
        for i, p in enumerate([me] + alike)
        for j, c in enumerate(columns)
    ]
    across_chip = [
        pltpu.make_async_remote_copy(
            routed.at[p], routed.at[p], c_send.at[i], c_recv.at[i],
            device_id=(mine, beside), device_id_type=MESH,
        )
        for i, p in enumerate([me] + alike)
    ]

    for s in range(LOADS):
        load(jnp.int32(s), True)
    load(jnp.int32(0), False)
    summed(jnp.int32(0))
    load(jnp.int32(LOADS), True)
    pl.semaphore_wait(barrier, len(peers) + len(columns))
    start(direct(0))

    @pl.loop(1, lead)
    def _(s):
        load(s, False)
        summed(s)
        load(s + LOADS, True)

    start(direct(1))
    start(fetch)

    @pl.loop(0, units)
    def _(i):
        def within(s):
            return (s >= lead) & (s < units)

        @pl.when(i >= WINDOW)
        def _():
            finish(far(i - WINDOW))

        @pl.when(i == 0)
        def _():
            finish(direct(0))
            early_total(0, 1)

        @pl.when(i == 1)
        def _():
            finish(direct(1))
            early_total(1, lead)

        @pl.when(i >= lead)
        def _():
            halves(i).wait()

        scaled(i)
        ahead = i + lead

        @pl.when(ahead < units)
        def _():
            load(ahead, False)
            summed(ahead)

        @pl.when(within(ahead - X_LAG))
        def _():
            s = ahead - X_LAG
            pair(s).wait()
            chip[s, 0] = part[s, core] + partner[s]

        @pl.when(within(ahead - Y_LAG))
        def _():
            s = ahead - Y_LAG
            chips(s, 0).wait()
            chip[s, 1] = chip[s, 0] + others[s, 0]

        @pl.when(within(ahead - HALF_LAG))
        def _():
            s = ahead - HALF_LAG
            chips(s, 1).wait()
            whole[s, core] = chip[s, 1] + others[s, 1]

        @pl.when(i == 2)
        def _():
            finish(fetch)
            routed[me, mine] = (weight[...] * gains[...]).astype(jnp.bfloat16)

        @pl.when(ahead < units)
        def _():
            pair(ahead).start()

        @pl.when(within(ahead - X_LAG))
        def _():
            chips(ahead - X_LAG, 0).start()

        @pl.when(within(ahead - Y_LAG))
        def _():
            chips(ahead - Y_LAG, 1).start()

        @pl.when(within(ahead - HALF_LAG))
        def _():
            halves(ahead - HALF_LAG).start()

        start(far(i))
        load(ahead + LOADS, True)

        @pl.when(i == 3)
        def _():
            start(along_rows)

        @pl.when(i == units // 4)
        def _():
            finish(along_rows)
            start(along_z)

        @pl.when(i == units // 2)
        def _():
            finish(along_z)
            start(across_chip)

        @pl.when(i == units - units // 4)
        def _():
            finish(across_chip)

    @pl.loop(max(units - WINDOW, 0), units)
    def _(s):
        finish(far(s))


def write_out(
    n, pieces, routed, scales, gate_out, up_out, gate_scale, up_scale, router_out,
    own, table, sems, small,
):
    experts, piece, rest = gate_out.shape[0], gate_out.shape[1], routed.shape[3]
    group = experts // WRITES
    big = [
        pltpu.make_async_copy(
            pieces.at[pl.ds(first + g * group, group)], target.at[pl.ds(g * group, group)],
            sems.at[first // experts, g],
        )
        for target, first in ((gate_out, 0), (up_out, experts))
        for g in range(WRITES)
    ]
    for copy in big:
        copy.start()
    me = lax.axis_index("rows")
    for p in range(n):
        block = routed[p].astype(jnp.float32).reshape(-1, rest)
        table[p * rest : (p + 1) * rest, :] = block.T.astype(jnp.bfloat16)

        @pl.when(me == p)
        def _():
            own[...] = scales[:, 0, p * piece : (p + 1) * piece]

    little = [
        pltpu.make_async_copy(table, router_out, small.at[0]),
        pltpu.make_async_copy(own.at[pl.ds(0, experts)], gate_scale, small.at[1]),
        pltpu.make_async_copy(own.at[pl.ds(experts, experts)], up_scale, small.at[2]),
    ]
    for copy in little:
        copy.start()
    for copy in little + big:
        copy.wait()


def in_kernels(n, owners, w_gate, w_up, router_weight, router_gain):
    experts, rows, width = w_gate.shape
    piece, units, across = width // n, 2 * experts, router_weight.shape[1]
    depth = n * rows
    steps = [1 << b for b in range(1, n.bit_length() - 1)]
    half = width // 2
    anywhere, vmem = pl.BlockSpec(memory_space=pl.ANY), pl.BlockSpec(memory_space=pltpu.VMEM)
    hbm, dma = pl.BlockSpec(memory_space=pltpu.HBM), pltpu.SemaphoreType.DMA
    pieces, routed, scales = pl.pallas_call(
        functools.partial(exchange, experts, n, owners, float(depth), steps),
        out_shape=(
            pltpu.VMEM((units, piece, depth), jnp.bfloat16),
            pltpu.VMEM((n, owners, across, rows), jnp.bfloat16),
            pltpu.VMEM((units, 1, width), jnp.float32),
        ),
        in_specs=[anywhere, anywhere, hbm, hbm],
        out_specs=(vmem, vmem, vmem),
        scratch_shapes=[
            pltpu.VMEM((HELD, rows, width), jnp.float32),
            pltpu.VMEM((WINDOW, width, rows), jnp.bfloat16),
            pltpu.VMEM((across, rows), jnp.float32),
            pltpu.VMEM((1, rows), jnp.float32),
            pltpu.VMEM((units, 2, 1, half), jnp.float32),
            pltpu.VMEM((n, LEAD, 2, 1, half), jnp.float32),
            pltpu.VMEM((units, 1, half), jnp.float32),
            pltpu.VMEM((units, 2, 1, half), jnp.float32),
            pltpu.VMEM((units, 2, 1, half), jnp.float32),
            pltpu.VMEM((units, 2, 1, half), jnp.float32),
            dma((HELD,)), dma((WINDOW, n - 1)), dma((2 * WINDOW, n - 1)),
            dma((SUMS,)), dma((SUMS,)), dma((SUMS, 2)), dma((SUMS, 2)), dma((SUMS,)), dma((SUMS,)),
            dma((2, n - 1)), dma((2, n - 1)), dma((2,)),
            dma((n // 2,)), dma((n // 2,)), dma((n // 2, owners)), dma((n // 2, owners)),
            dma((n // 2,)), dma((n // 2,)),
        ],
        compiler_params=pltpu.CompilerParams(
            collective_id=0, has_side_effects=True, vmem_limit_bytes=12 * 2**20
        ),
        name="exchange",
    )(w_gate, w_up, *(pltpu.with_memory_space_constraint(x, pltpu.HBM) for x in (router_weight.T, router_gain[None, :])))

    gate, up, gate_scale, up_scale, router = pl.pallas_call(
        functools.partial(write_out, n),
        out_shape=(
            jax.ShapeDtypeStruct((experts, piece, depth), jnp.bfloat16),
            jax.ShapeDtypeStruct((experts, piece, depth), jnp.bfloat16),
            jax.ShapeDtypeStruct((experts, piece), jnp.float32),
            jax.ShapeDtypeStruct((experts, piece), jnp.float32),
            jax.ShapeDtypeStruct((depth, owners * across), jnp.bfloat16),
        ),
        in_specs=[vmem, vmem, vmem],
        out_specs=(anywhere,) * 5,
        scratch_shapes=[
            pltpu.VMEM((units, piece), jnp.float32),
            pltpu.VMEM((depth, owners * across), jnp.bfloat16),
            dma((2, WRITES)), dma((3,)),
        ],
        compiler_params=pltpu.CompilerParams(vmem_limit_bytes=1 * 2**20),
        name="write_out",
    )(*(pltpu.with_memory_space_constraint(x, pltpu.VMEM) for x in (pieces, routed, scales)))
    return jnp.swapaxes(gate, 1, 2), jnp.swapaxes(up, 1, 2), gate_scale, up_scale, router


def in_ops(n, w_gate, w_up, router_weight, router_gain):
    depth = n * w_gate.shape[1]
    sums = (jnp.sum(jnp.abs(w_gate), axis=1), jnp.sum(jnp.abs(w_up), axis=1))
    served, scales = [], []
    for w, total in zip((w_gate, w_up), lax.psum(sums, "rows")):
        scale = total / depth
        narrow = (w / jnp.expand_dims(scale, 1)).astype(jnp.bfloat16)
        piece = lax.all_to_all(narrow, "rows", split_axis=2, concat_axis=1, tiled=True)
        size = piece.shape[2]
        served.append(piece)
        scales.append(lax.dynamic_slice_in_dim(scale, lax.axis_index("rows") * size, size, axis=1))
    part = (router_weight * router_gain[:, None]).astype(jnp.bfloat16)
    router = lax.all_gather(part, "rows", axis=0, tiled=True)
    router = lax.all_gather(router, "owner", axis=1, tiled=True)
    return (*served, *scales, router)


def solution(mesh):
    n, owners = mesh.shape["rows"], mesh.shape["owner"]

    def on_device(w_gate, w_up, router_weight, router_gain):
        experts, rows, width = w_gate.shape
        whole_tiles = (
            rows % 128 == 0 and width % (16 * n) == 0 and width % 256 == 0
            and n == 8 and owners > 1 and experts % WRITES == 0 and 2 * experts >= 2 * LEAD
        )
        if whole_tiles:
            return in_kernels(n, owners, w_gate, w_up, router_weight, router_gain)
        return in_ops(n, w_gate, w_up, router_weight, router_gain)

    placed = (P("owner", "rows", None), P("owner", "rows", None), P("rows", "owner"), P("rows"))
    return jax.shard_map(
        on_device,
        mesh=mesh,
        in_specs=placed,
        out_specs=(
            P("owner", None, "rows"),
            P("owner", None, "rows"),
            P("owner", "rows"),
            P("owner", "rows"),
            P(),
        ),
        check_vma=False,
    )
```

```python
import functools

import jax
import jax.numpy as jnp
from jax import lax
from jax.experimental import pallas as pl
from jax.experimental.pallas import tpu as pltpu
from jax.sharding import PartitionSpec as P

MESH = pl.DeviceIdType.MESH
WINDOW = 3
LOADS = 3
LEAD = 6
X_LAG, Y_LAG, HALF_LAG = 1, 3, 5
HELD = LOADS + LEAD
SUMS = 2 * LEAD + 2
WRITES = 4


def peer_steps(n):
    far = list(range(2, n, 2))
    return far + [k + 1 for k in far] + [1]


def toggled(index, k):
    result, bit = index, 1
    while bit <= k:
        if k & bit:
            result = result + bit * (1 - 2 * lax.rem(index // bit, 2))
        bit *= 2
    return result


def exchange(
    experts, n, owners, depth, steps,
    gate, up, router, gain,
    pieces, routed, scales,
    window, stage, weight, gains, part, early, partner, chip, others, whole,
    load_sem, send_sem, recv_sem, pair_send, pair_recv, sum_send, sum_recv, last_send, last_recv,
    early_send, early_recv, in_sem, r_send, r_recv, z_send, z_recv, c_send, c_recv,
):
    me, mine = lax.axis_index("rows"), lax.axis_index("owner")
    units, piece, rows, width = 2 * experts, pieces.shape[1], gate.shape[1], gate.shape[2]
    lead = early.shape[1]
    peers = [toggled(me, k) for k in peer_steps(n)]
    alike = [toggled(me, k) for k in range(2, n, 2)]
    core, beside = lax.rem(me, 2), toggled(me, 1)
    below, above = lax.max(mine - 1, 0), lax.min(mine + 1, owners - 1)

    barrier = pltpu.get_barrier_semaphore()
    for p in peers:
        pl.semaphore_signal(barrier, inc=1, device_id=(mine, p), device_id_type=MESH)

    @pl.when(mine < owners - 1)
    def _():
        pl.semaphore_signal(barrier, inc=1, device_id=(above, me), device_id_type=MESH)

    def load(s, go):
        for matrix, first in ((gate, 0), (up, experts)):
            @pl.when((s >= first) & (s < first + experts))
            def _():
                slot = lax.rem(s, HELD)
                copy = pltpu.make_async_copy(matrix.at[s - first], window.at[slot], load_sem.at[slot])
                copy.start() if go else copy.wait()

    def pair(s):
        slot = lax.rem(s, SUMS)
        return pltpu.make_async_remote_copy(
            part.at[s, 1 - core], partner.at[s], pair_send.at[slot], pair_recv.at[slot],
            device_id=(mine, beside), device_id_type=MESH,
        )

    def chips(s, t):
        slot = lax.rem(s, SUMS)
        return pltpu.make_async_remote_copy(
            chip.at[s, t], others.at[s, t], sum_send.at[slot, t], sum_recv.at[slot, t],
            device_id=(mine, toggled(me, steps[t])), device_id_type=MESH,
        )

    def halves(s):
        slot = lax.rem(s, SUMS)
        return pltpu.make_async_remote_copy(
            whole.at[s, core], whole.at[s, core], last_send.at[slot], last_recv.at[slot],
            device_id=(mine, beside), device_id_type=MESH,
        )

    def direct(g):
        first, count = ((0, 1), (1, lead - 1))[g]
        return [
            pltpu.make_async_remote_copy(
                part.at[pl.ds(first, count)], early.at[me, pl.ds(first, count)],
                early_send.at[g, i], early_recv.at[g, i],
                device_id=(mine, p), device_id_type=MESH,
            )
            for i, p in enumerate(peers)
        ]

    def far(s):
        slot, land = lax.rem(s, WINDOW), lax.rem(s, 2 * WINDOW)
        return [
            pltpu.make_async_remote_copy(
                stage.at[slot, pl.ds(pl.multiple_of(p * piece, piece), piece)],
                pieces.at[s, :, pl.ds(pl.multiple_of(me * rows, rows), rows)],
                send_sem.at[slot, i], recv_sem.at[land, i],
                device_id=(mine, p), device_id_type=MESH,
            )
            for i, p in enumerate(peers)
        ]

    def start(copies):
        for copy in copies:
            copy.start()

    def finish(copies):
        for copy in copies:
            copy.wait()

    def summed(s):
        half = width // 2
        for h in range(2):
            w = window[lax.rem(s, HELD), :, h * half : (h + 1) * half]
            part[s, h] = jnp.sum(jnp.abs(w), axis=0, keepdims=True)

    def early_total(first, last):
        for h in range(2):
            total = jnp.zeros((last - first, 1, width // 2), jnp.float32)
            for p in range(n):
                total = total + jnp.where(p == me, part[first:last, h], early[p, first:last, h])
            whole[first:last, h] = total

    def scaled(s):
        slot, held = lax.rem(s, WINDOW), lax.rem(s, HELD)
        scale = jnp.concatenate([whole[s, 0], whole[s, 1]], axis=1) / depth
        scales[s] = scale
        inverse = 1.0 / scale
        for at in range(0, width, 128):
            w = window[held, :, at : at + 128] * inverse[:, at : at + 128]
            stage[slot, at : at + 128, :] = w.T.astype(jnp.bfloat16)
        own = stage[slot, pl.ds(pl.multiple_of(me * piece, piece), piece), :]
        pieces[s, :, pl.ds(pl.multiple_of(me * rows, rows), rows)] = own

    fetch = [
        pltpu.make_async_copy(router, weight, in_sem.at[0]),
        pltpu.make_async_copy(gain, gains, in_sem.at[1]),
    ]
    along_rows = [
        pltpu.make_async_remote_copy(
            routed.at[me, mine], routed.at[me, mine], r_send.at[i], r_recv.at[i],
            device_id=(mine, p), device_id_type=MESH,
        )
        for i, p in enumerate(alike)
    ]
    mates = [me] + alike

    def relay(up, step):
        block, side = (mine - step, 1) if up else (mine + step, 0)
        block = lax.max(lax.min(block, owners - 1), 0)
        return [
            pltpu.make_async_remote_copy(
                routed.at[p, block], routed.at[p, block],
                z_send.at[side, step, i], z_recv.at[side, step, i],
                device_id=(above if up else below, me), device_id_type=MESH,
            )
            for i, p in enumerate(mates)
        ]

    def arrival(up, step):
        block, side = (mine - 1 - step, 1) if up else (mine + 1 + step, 0)
        block = lax.max(lax.min(block, owners - 1), 0)
        return [
            pltpu.make_async_remote_copy(
                routed.at[p, block], routed.at[p, block],
                z_send.at[side, step, i], z_recv.at[side, step, i],
                device_id=(above if up else below, me), device_id_type=MESH,
            )
            for i, p in enumerate(mates)
        ]

    def relays(turn):
        for up, step in ((False, turn - 1), (True, turn - 2)):
            if 0 <= step < owners - 1:
                came = (mine > step) if up else (mine + step < owners - 1)
                went = (mine < owners - 1) & (mine >= step) if up else (mine > 0) & (mine + step <= owners - 1)

                @pl.when(came)
                def _():
                    for copy in arrival(up, step):
                        copy.wait_recv()

                @pl.when(went)
                def _():
                    for copy in relay(up, step):
                        copy.wait_send()
        for up, step in ((False, turn), (True, turn - 1)):
            if 0 <= step < owners - 1:
                went = (mine < owners - 1) & (mine >= step) if up else (mine > 0) & (mine + step <= owners - 1)

                @pl.when(went)
                def _():
                    start(relay(up, step))

    across_chip = [
        pltpu.make_async_remote_copy(
            routed.at[p], routed.at[p], c_send.at[i], c_recv.at[i],
            device_id=(mine, beside), device_id_type=MESH,
        )
        for i, p in enumerate(mates)
    ]

    start(fetch)
    for s in range(LOADS):
        load(jnp.int32(s), True)
    load(jnp.int32(0), False)
    summed(jnp.int32(0))
    load(jnp.int32(LOADS), True)
    finish(fetch)
    routed[me, mine] = (weight[...] * gains[...]).astype(jnp.bfloat16)
    pl.semaphore_wait(barrier, len(peers) + jnp.where(mine > 0, 1, 0))
    start(direct(0))

    @pl.loop(1, lead)
    def _(s):
        load(s, False)
        summed(s)
        load(s + LOADS, True)

    start(direct(1))
    start(along_rows)

    @pl.loop(0, units)
    def _(i):
        def within(s):
            return (s >= lead) & (s < units)

        @pl.when(i >= WINDOW)
        def _():
            finish(far(i - WINDOW))

        @pl.when(i == 0)
        def _():
            finish(direct(0))
            early_total(0, 1)

        @pl.when(i == 1)
        def _():
            finish(direct(1))
            early_total(1, lead)

        @pl.when(i >= lead)
        def _():
            halves(i).wait()

        scaled(i)
        ahead = i + lead

        @pl.when(ahead < units)
        def _():
            load(ahead, False)
            summed(ahead)

        @pl.when(within(ahead - X_LAG))
        def _():
            s = ahead - X_LAG
            pair(s).wait()
            chip[s, 0] = part[s, core] + partner[s]

        @pl.when(within(ahead - Y_LAG))
        def _():
            s = ahead - Y_LAG
            chips(s, 0).wait()
            chip[s, 1] = chip[s, 0] + others[s, 0]

        @pl.when(within(ahead - HALF_LAG))
        def _():
            s = ahead - HALF_LAG
            chips(s, 1).wait()
            whole[s, core] = chip[s, 1] + others[s, 1]

        @pl.when(ahead < units)
        def _():
            pair(ahead).start()

        @pl.when(within(ahead - X_LAG))
        def _():
            chips(ahead - X_LAG, 0).start()

        @pl.when(within(ahead - Y_LAG))
        def _():
            chips(ahead - Y_LAG, 1).start()

        @pl.when(within(ahead - HALF_LAG))
        def _():
            halves(ahead - HALF_LAG).start()

        start(far(i))
        load(ahead + LOADS, True)

        @pl.when(i == LEAD)
        def _():
            finish(along_rows)

        for turn in range(owners + 1):
            @pl.when(i == LEAD + 1 + 2 * turn)
            def _():
                relays(turn)

        @pl.when(i == units // 2)
        def _():
            start(across_chip)

        @pl.when(i == units - units // 4)
        def _():
            finish(across_chip)

    @pl.loop(max(units - WINDOW, 0), units)
    def _(s):
        finish(far(s))


def write_out(
    n, pieces, routed, scales, gate_out, up_out, gate_scale, up_scale, router_out,
    own, table, sems, small,
):
    experts, piece, rest = gate_out.shape[0], gate_out.shape[1], routed.shape[3]
    group = experts // WRITES
    big = [
        pltpu.make_async_copy(
            pieces.at[pl.ds(first + g * group, group)], target.at[pl.ds(g * group, group)],
            sems.at[first // experts, g],
        )
        for target, first in ((gate_out, 0), (up_out, experts))
        for g in range(WRITES)
    ]
    for copy in big:
        copy.start()
    me = lax.axis_index("rows")
    for p in range(n):
        block = routed[p].astype(jnp.float32).reshape(-1, rest)
        table[p * rest : (p + 1) * rest, :] = block.T.astype(jnp.bfloat16)

        @pl.when(me == p)
        def _():
            own[...] = scales[:, 0, p * piece : (p + 1) * piece]

    little = [
        pltpu.make_async_copy(table, router_out, small.at[0]),
        pltpu.make_async_copy(own.at[pl.ds(0, experts)], gate_scale, small.at[1]),
        pltpu.make_async_copy(own.at[pl.ds(experts, experts)], up_scale, small.at[2]),
    ]
    for copy in little:
        copy.start()
    for copy in little + big:
        copy.wait()


def in_kernels(n, owners, w_gate, w_up, router_weight, router_gain):
    experts, rows, width = w_gate.shape
    piece, units, across = width // n, 2 * experts, router_weight.shape[1]
    depth = n * rows
    steps = [1 << b for b in range(1, n.bit_length() - 1)]
    half = width // 2
    anywhere, vmem = pl.BlockSpec(memory_space=pl.ANY), pl.BlockSpec(memory_space=pltpu.VMEM)
    hbm, dma = pl.BlockSpec(memory_space=pltpu.HBM), pltpu.SemaphoreType.DMA
    pieces, routed, scales = pl.pallas_call(
        functools.partial(exchange, experts, n, owners, float(depth), steps),
        out_shape=(
            pltpu.VMEM((units, piece, depth), jnp.bfloat16),
            pltpu.VMEM((n, owners, across, rows), jnp.bfloat16),
            pltpu.VMEM((units, 1, width), jnp.float32),
        ),
        in_specs=[anywhere, anywhere, hbm, hbm],
        out_specs=(vmem, vmem, vmem),
        scratch_shapes=[
            pltpu.VMEM((HELD, rows, width), jnp.float32),
            pltpu.VMEM((WINDOW, width, rows), jnp.bfloat16),
            pltpu.VMEM((across, rows), jnp.float32),
            pltpu.VMEM((1, rows), jnp.float32),
            pltpu.VMEM((units, 2, 1, half), jnp.float32),
            pltpu.VMEM((n, LEAD, 2, 1, half), jnp.float32),
            pltpu.VMEM((units, 1, half), jnp.float32),
            pltpu.VMEM((units, 2, 1, half), jnp.float32),
            pltpu.VMEM((units, 2, 1, half), jnp.float32),
            pltpu.VMEM((units, 2, 1, half), jnp.float32),
            dma((HELD,)), dma((WINDOW, n - 1)), dma((2 * WINDOW, n - 1)),
            dma((SUMS,)), dma((SUMS,)), dma((SUMS, 2)), dma((SUMS, 2)), dma((SUMS,)), dma((SUMS,)),
            dma((2, n - 1)), dma((2, n - 1)), dma((2,)),
            dma((n // 2,)), dma((n // 2,)), dma((2, owners, n // 2)), dma((2, owners, n // 2)),
            dma((n // 2,)), dma((n // 2,)),
        ],
        compiler_params=pltpu.CompilerParams(
            collective_id=0, has_side_effects=True, vmem_limit_bytes=12 * 2**20
        ),
        name="exchange",
    )(w_gate, w_up, *(pltpu.with_memory_space_constraint(x, pltpu.HBM) for x in (router_weight.T, router_gain[None, :])))

    gate, up, gate_scale, up_scale, router = pl.pallas_call(
        functools.partial(write_out, n),
        out_shape=(
            jax.ShapeDtypeStruct((experts, piece, depth), jnp.bfloat16),
            jax.ShapeDtypeStruct((experts, piece, depth), jnp.bfloat16),
            jax.ShapeDtypeStruct((experts, piece), jnp.float32),
            jax.ShapeDtypeStruct((experts, piece), jnp.float32),
            jax.ShapeDtypeStruct((depth, owners * across), jnp.bfloat16),
        ),
        in_specs=[vmem, vmem, vmem],
        out_specs=(anywhere,) * 5,
        scratch_shapes=[
            pltpu.VMEM((units, piece), jnp.float32),
            pltpu.VMEM((depth, owners * across), jnp.bfloat16),
            dma((2, WRITES)), dma((3,)),
        ],
        compiler_params=pltpu.CompilerParams(vmem_limit_bytes=1 * 2**20),
        name="write_out",
    )(*(pltpu.with_memory_space_constraint(x, pltpu.VMEM) for x in (pieces, routed, scales)))
    return jnp.swapaxes(gate, 1, 2), jnp.swapaxes(up, 1, 2), gate_scale, up_scale, router


def in_ops(n, w_gate, w_up, router_weight, router_gain):
    depth = n * w_gate.shape[1]
    sums = (jnp.sum(jnp.abs(w_gate), axis=1), jnp.sum(jnp.abs(w_up), axis=1))
    served, scales = [], []
    for w, total in zip((w_gate, w_up), lax.psum(sums, "rows")):
        scale = total / depth
        narrow = (w / jnp.expand_dims(scale, 1)).astype(jnp.bfloat16)
        piece = lax.all_to_all(narrow, "rows", split_axis=2, concat_axis=1, tiled=True)
        size = piece.shape[2]
        served.append(piece)
        scales.append(lax.dynamic_slice_in_dim(scale, lax.axis_index("rows") * size, size, axis=1))
    part = (router_weight * router_gain[:, None]).astype(jnp.bfloat16)
    router = lax.all_gather(part, "rows", axis=0, tiled=True)
    router = lax.all_gather(router, "owner", axis=1, tiled=True)
    return (*served, *scales, router)


def solution(mesh):
    n, owners = mesh.shape["rows"], mesh.shape["owner"]

    def on_device(w_gate, w_up, router_weight, router_gain):
        experts, rows, width = w_gate.shape
        whole_tiles = (
            rows % 128 == 0 and width % (16 * n) == 0 and width % 256 == 0
            and n == 8 and owners > 1 and experts % WRITES == 0 and experts >= LEAD + 3 + 2 * owners
        )
        if whole_tiles:
            return in_kernels(n, owners, w_gate, w_up, router_weight, router_gain)
        return in_ops(n, w_gate, w_up, router_weight, router_gain)

    placed = (P("owner", "rows", None), P("owner", "rows", None), P("rows", "owner"), P("rows"))
    return jax.shard_map(
        on_device,
        mesh=mesh,
        in_specs=placed,
        out_specs=(
            P("owner", None, "rows"),
            P("owner", None, "rows"),
            P("owner", "rows"),
            P("owner", "rows"),
            P(),
        ),
        check_vma=False,
    )
```

```python
import functools

import jax
import jax.numpy as jnp
from jax import lax
from jax.experimental import pallas as pl
from jax.experimental.pallas import tpu as pltpu
from jax.sharding import PartitionSpec as P

MESH = pl.DeviceIdType.MESH
WINDOW = 2
LOADS = 3
LEAD = 4
X_LAG, Y_LAG, HALF_LAG = 1, 2, 3
HELD = LOADS + LEAD
SUMS = 2 * LEAD + 2
WRITES = 4


def peer_steps(n):
    far = list(range(2, n, 2))
    return far + [k + 1 for k in far] + [1]


def toggled(index, k):
    result, bit = index, 1
    while bit <= k:
        if k & bit:
            result = result + bit * (1 - 2 * lax.rem(index // bit, 2))
        bit *= 2
    return result


def exchange(
    experts, n, owners, depth, steps,
    gate, up, router, gain,
    pieces, routed, scales,
    window, stage, weight, gains, part, early, partner, chip, others, whole,
    load_sem, send_sem, recv_sem, pair_send, pair_recv, sum_send, sum_recv, last_send, last_recv,
    early_send, early_recv, in_sem, r_send, r_recv, z_send, z_recv, c_send, c_recv,
):
    me, mine = lax.axis_index("rows"), lax.axis_index("owner")
    units, piece, rows, width = 2 * experts, pieces.shape[1], gate.shape[1], gate.shape[2]
    lead = early.shape[1]
    peers = [toggled(me, k) for k in peer_steps(n)]
    alike = [toggled(me, k) for k in range(2, n, 2)]
    core, beside = lax.rem(me, 2), toggled(me, 1)
    below, above = lax.max(mine - 1, 0), lax.min(mine + 1, owners - 1)

    barrier = pltpu.get_barrier_semaphore()
    for p in peers:
        pl.semaphore_signal(barrier, inc=1, device_id=(mine, p), device_id_type=MESH)

    @pl.when(mine < owners - 1)
    def _():
        pl.semaphore_signal(barrier, inc=1, device_id=(above, me), device_id_type=MESH)

    def load(s, go):
        for matrix, first in ((gate, 0), (up, experts)):
            @pl.when((s >= first) & (s < first + experts))
            def _():
                slot = lax.rem(s, HELD)
                copy = pltpu.make_async_copy(matrix.at[s - first], window.at[slot], load_sem.at[slot])
                copy.start() if go else copy.wait()

    def pair(s):
        slot = lax.rem(s, SUMS)
        return pltpu.make_async_remote_copy(
            part.at[s, 1 - core], partner.at[s], pair_send.at[slot], pair_recv.at[slot],
            device_id=(mine, beside), device_id_type=MESH,
        )

    def chips(s, t):
        slot = lax.rem(s, SUMS)
        return pltpu.make_async_remote_copy(
            chip.at[s, t], others.at[s, t], sum_send.at[slot, t], sum_recv.at[slot, t],
            device_id=(mine, toggled(me, steps[t])), device_id_type=MESH,
        )

    def halves(s):
        slot = lax.rem(s, SUMS)
        return pltpu.make_async_remote_copy(
            whole.at[s, core], whole.at[s, core], last_send.at[slot], last_recv.at[slot],
            device_id=(mine, beside), device_id_type=MESH,
        )

    def direct(g):
        first, count = ((0, 1), (1, lead - 1))[g]
        return [
            pltpu.make_async_remote_copy(
                part.at[pl.ds(first, count)], early.at[me, pl.ds(first, count)],
                early_send.at[g, i], early_recv.at[g, i],
                device_id=(mine, p), device_id_type=MESH,
            )
            for i, p in enumerate(peers)
        ]

    def far(s):
        slot, land = lax.rem(s, WINDOW), lax.rem(s, 2 * WINDOW)
        return [
            pltpu.make_async_remote_copy(
                stage.at[slot, pl.ds(pl.multiple_of(p * piece, piece), piece)],
                pieces.at[s, :, pl.ds(pl.multiple_of(me * rows, rows), rows)],
                send_sem.at[slot, i], recv_sem.at[land, i],
                device_id=(mine, p), device_id_type=MESH,
            )
            for i, p in enumerate(peers)
        ]

    def start(copies):
        for copy in copies:
            copy.start()

    def finish(copies):
        for copy in copies:
            copy.wait()

    def summed(s):
        half = width // 2
        for h in range(2):
            w = window[lax.rem(s, HELD), :, h * half : (h + 1) * half]
            part[s, h] = jnp.sum(jnp.abs(w), axis=0, keepdims=True)

    def early_total(first, last):
        for h in range(2):
            total = jnp.zeros((last - first, 1, width // 2), jnp.float32)
            for p in range(n):
                total = total + jnp.where(p == me, part[first:last, h], early[p, first:last, h])
            whole[first:last, h] = total

    def scaled(s):
        slot, held = lax.rem(s, WINDOW), lax.rem(s, HELD)
        scale = jnp.concatenate([whole[s, 0], whole[s, 1]], axis=1) / depth
        scales[s] = scale
        inverse = 1.0 / scale
        for at in range(0, width, 128):
            w = window[held, :, at : at + 128] * inverse[:, at : at + 128]
            stage[slot, at : at + 128, :] = w.T.astype(jnp.bfloat16)
        own = stage[slot, pl.ds(pl.multiple_of(me * piece, piece), piece), :]
        pieces[s, :, pl.ds(pl.multiple_of(me * rows, rows), rows)] = own

    fetch = [
        pltpu.make_async_copy(router, weight, in_sem.at[0]),
        pltpu.make_async_copy(gain, gains, in_sem.at[1]),
    ]
    along_rows = [
        pltpu.make_async_remote_copy(
            routed.at[me, mine], routed.at[me, mine], r_send.at[i], r_recv.at[i],
            device_id=(mine, p), device_id_type=MESH,
        )
        for i, p in enumerate(alike)
    ]
    mates = [me] + alike

    def relay(up, step):
        block, side = (mine - step, 1) if up else (mine + step, 0)
        block = lax.max(lax.min(block, owners - 1), 0)
        return [
            pltpu.make_async_remote_copy(
                routed.at[p, block], routed.at[p, block],
                z_send.at[side, step, i], z_recv.at[side, step, i],
                device_id=(above if up else below, me), device_id_type=MESH,
            )
            for i, p in enumerate(mates)
        ]

    def arrival(up, step):
        block, side = (mine - 1 - step, 1) if up else (mine + 1 + step, 0)
        block = lax.max(lax.min(block, owners - 1), 0)
        return [
            pltpu.make_async_remote_copy(
                routed.at[p, block], routed.at[p, block],
                z_send.at[side, step, i], z_recv.at[side, step, i],
                device_id=(above if up else below, me), device_id_type=MESH,
            )
            for i, p in enumerate(mates)
        ]

    def relays(turn):
        for up, step in ((False, turn - 1), (True, turn - 2)):
            if 0 <= step < owners - 1:
                came = (mine > step) if up else (mine + step < owners - 1)
                went = (mine < owners - 1) & (mine >= step) if up else (mine > 0) & (mine + step <= owners - 1)

                @pl.when(came)
                def _():
                    for copy in arrival(up, step):
                        copy.wait_recv()

                @pl.when(went)
                def _():
                    for copy in relay(up, step):
                        copy.wait_send()
        for up, step in ((False, turn), (True, turn - 1)):
            if 0 <= step < owners - 1:
                went = (mine < owners - 1) & (mine >= step) if up else (mine > 0) & (mine + step <= owners - 1)

                @pl.when(went)
                def _():
                    start(relay(up, step))

    across_chip = [
        pltpu.make_async_remote_copy(
            routed.at[p], routed.at[p], c_send.at[i], c_recv.at[i],
            device_id=(mine, beside), device_id_type=MESH,
        )
        for i, p in enumerate(mates)
    ]

    load(jnp.int32(0), True)
    start(fetch)
    load(jnp.int32(0), False)
    summed(jnp.int32(0))
    pl.semaphore_wait(barrier, len(peers) + jnp.where(mine > 0, 1, 0))
    start(direct(0)[::-1])

    @pl.loop(1, HELD)
    def _(s):
        load(s, True)

    finish(fetch)
    routed[me, mine] = (weight[...] * gains[...]).astype(jnp.bfloat16)

    @pl.loop(1, lead)
    def _(s):
        load(s, False)
        summed(s)

    start(direct(1))
    start(along_rows)

    @pl.loop(0, units)
    def _(i):
        def within(s):
            return (s >= lead) & (s < units)

        @pl.when(i >= WINDOW)
        def _():
            finish(far(i - WINDOW))

        @pl.when(i == 0)
        def _():
            finish(direct(0))
            early_total(0, 1)

        @pl.when(i == 1)
        def _():
            finish(direct(1))
            early_total(1, lead)

        @pl.when(i >= lead)
        def _():
            halves(i).wait()

        scaled(i)
        ahead = i + lead

        @pl.when(ahead < units)
        def _():
            load(ahead, False)
            summed(ahead)

        @pl.when(within(ahead - X_LAG))
        def _():
            s = ahead - X_LAG
            pair(s).wait()
            chip[s, 0] = part[s, core] + partner[s]

        @pl.when(within(ahead - Y_LAG))
        def _():
            s = ahead - Y_LAG
            chips(s, 0).wait()
            chip[s, 1] = chip[s, 0] + others[s, 0]

        @pl.when(within(ahead - HALF_LAG))
        def _():
            s = ahead - HALF_LAG
            chips(s, 1).wait()
            whole[s, core] = chip[s, 1] + others[s, 1]

        @pl.when(ahead < units)
        def _():
            pair(ahead).start()

        @pl.when(within(ahead - X_LAG))
        def _():
            chips(ahead - X_LAG, 0).start()

        @pl.when(within(ahead - Y_LAG))
        def _():
            chips(ahead - Y_LAG, 1).start()

        @pl.when(within(ahead - HALF_LAG))
        def _():
            halves(ahead - HALF_LAG).start()

        start(far(i))
        load(ahead + LOADS, True)

        @pl.when(i == LEAD)
        def _():
            finish(along_rows)

        for turn in range(owners + 1):
            @pl.when(i == LEAD + 1 + 2 * turn)
            def _():
                relays(turn)

        @pl.when(i == units // 2)
        def _():
            start(across_chip)

        @pl.when(i == units - units // 4)
        def _():
            finish(across_chip)

    @pl.loop(max(units - WINDOW, 0), units)
    def _(s):
        finish(far(s))


def write_out(
    n, pieces, routed, scales, gate_out, up_out, gate_scale, up_scale, router_out,
    own, table, sems, small,
):
    experts, piece, rest = gate_out.shape[0], gate_out.shape[1], routed.shape[3]
    group = experts // WRITES
    big = [
        pltpu.make_async_copy(
            pieces.at[pl.ds(first + g * group, group)], target.at[pl.ds(g * group, group)],
            sems.at[first // experts, g],
        )
        for target, first in ((gate_out, 0), (up_out, experts))
        for g in range(WRITES)
    ]
    for copy in big:
        copy.start()
    me = lax.axis_index("rows")
    for p in range(n):
        block = routed[p].astype(jnp.float32).reshape(-1, rest)
        table[p * rest : (p + 1) * rest, :] = block.T.astype(jnp.bfloat16)

        @pl.when(me == p)
        def _():
            own[...] = scales[:, 0, p * piece : (p + 1) * piece]

    little = [
        pltpu.make_async_copy(table, router_out, small.at[0]),
        pltpu.make_async_copy(own.at[pl.ds(0, experts)], gate_scale, small.at[1]),
        pltpu.make_async_copy(own.at[pl.ds(experts, experts)], up_scale, small.at[2]),
    ]
    for copy in little:
        copy.start()
    for copy in little + big:
        copy.wait()


def in_kernels(n, owners, w_gate, w_up, router_weight, router_gain):
    experts, rows, width = w_gate.shape
    piece, units, across = width // n, 2 * experts, router_weight.shape[1]
    depth = n * rows
    steps = [1 << b for b in range(1, n.bit_length() - 1)]
    half = width // 2
    anywhere, vmem = pl.BlockSpec(memory_space=pl.ANY), pl.BlockSpec(memory_space=pltpu.VMEM)
    hbm, dma = pl.BlockSpec(memory_space=pltpu.HBM), pltpu.SemaphoreType.DMA
    pieces, routed, scales = pl.pallas_call(
        functools.partial(exchange, experts, n, owners, float(depth), steps),
        out_shape=(
            pltpu.VMEM((units, piece, depth), jnp.bfloat16),
            pltpu.VMEM((n, owners, across, rows), jnp.bfloat16),
            pltpu.VMEM((units, 1, width), jnp.float32),
        ),
        in_specs=[anywhere, anywhere, hbm, hbm],
        out_specs=(vmem, vmem, vmem),
        scratch_shapes=[
            pltpu.VMEM((HELD, rows, width), jnp.float32),
            pltpu.VMEM((WINDOW, width, rows), jnp.bfloat16),
            pltpu.VMEM((across, rows), jnp.float32),
            pltpu.VMEM((1, rows), jnp.float32),
            pltpu.VMEM((units, 2, 1, half), jnp.float32),
            pltpu.VMEM((n, LEAD, 2, 1, half), jnp.float32),
            pltpu.VMEM((units, 1, half), jnp.float32),
            pltpu.VMEM((units, 2, 1, half), jnp.float32),
            pltpu.VMEM((units, 2, 1, half), jnp.float32),
            pltpu.VMEM((units, 2, 1, half), jnp.float32),
            dma((HELD,)), dma((WINDOW, n - 1)), dma((2 * WINDOW, n - 1)),
            dma((SUMS,)), dma((SUMS,)), dma((SUMS, 2)), dma((SUMS, 2)), dma((SUMS,)), dma((SUMS,)),
            dma((2, n - 1)), dma((2, n - 1)), dma((2,)),
            dma((n // 2,)), dma((n // 2,)), dma((2, owners, n // 2)), dma((2, owners, n // 2)),
            dma((n // 2,)), dma((n // 2,)),
        ],
        compiler_params=pltpu.CompilerParams(
            collective_id=0, has_side_effects=True, vmem_limit_bytes=12 * 2**20
        ),
        name="exchange",
    )(w_gate, w_up, *(pltpu.with_memory_space_constraint(x, pltpu.HBM) for x in (router_weight.T, router_gain[None, :])))

    gate, up, gate_scale, up_scale, router = pl.pallas_call(
        functools.partial(write_out, n),
        out_shape=(
            jax.ShapeDtypeStruct((experts, piece, depth), jnp.bfloat16),
            jax.ShapeDtypeStruct((experts, piece, depth), jnp.bfloat16),
            jax.ShapeDtypeStruct((experts, piece), jnp.float32),
            jax.ShapeDtypeStruct((experts, piece), jnp.float32),
            jax.ShapeDtypeStruct((depth, owners * across), jnp.bfloat16),
        ),
        in_specs=[vmem, vmem, vmem],
        out_specs=(anywhere,) * 5,
        scratch_shapes=[
            pltpu.VMEM((units, piece), jnp.float32),
            pltpu.VMEM((depth, owners * across), jnp.bfloat16),
            dma((2, WRITES)), dma((3,)),
        ],
        compiler_params=pltpu.CompilerParams(vmem_limit_bytes=1 * 2**20),
        name="write_out",
    )(*(pltpu.with_memory_space_constraint(x, pltpu.VMEM) for x in (pieces, routed, scales)))
    return jnp.swapaxes(gate, 1, 2), jnp.swapaxes(up, 1, 2), gate_scale, up_scale, router


def in_ops(n, w_gate, w_up, router_weight, router_gain):
    depth = n * w_gate.shape[1]
    sums = (jnp.sum(jnp.abs(w_gate), axis=1), jnp.sum(jnp.abs(w_up), axis=1))
    served, scales = [], []
    for w, total in zip((w_gate, w_up), lax.psum(sums, "rows")):
        scale = total / depth
        narrow = (w / jnp.expand_dims(scale, 1)).astype(jnp.bfloat16)
        piece = lax.all_to_all(narrow, "rows", split_axis=2, concat_axis=1, tiled=True)
        size = piece.shape[2]
        served.append(piece)
        scales.append(lax.dynamic_slice_in_dim(scale, lax.axis_index("rows") * size, size, axis=1))
    part = (router_weight * router_gain[:, None]).astype(jnp.bfloat16)
    router = lax.all_gather(part, "rows", axis=0, tiled=True)
    router = lax.all_gather(router, "owner", axis=1, tiled=True)
    return (*served, *scales, router)


def solution(mesh):
    n, owners = mesh.shape["rows"], mesh.shape["owner"]

    def on_device(w_gate, w_up, router_weight, router_gain):
        experts, rows, width = w_gate.shape
        whole_tiles = (
            rows % 128 == 0 and width % (16 * n) == 0 and width % 256 == 0
            and n == 8 and owners > 1 and experts % WRITES == 0 and experts >= LEAD + 3 + 2 * owners
        )
        if whole_tiles:
            return in_kernels(n, owners, w_gate, w_up, router_weight, router_gain)
        return in_ops(n, w_gate, w_up, router_weight, router_gain)

    placed = (P("owner", "rows", None), P("owner", "rows", None), P("rows", "owner"), P("rows"))
    return jax.shard_map(
        on_device,
        mesh=mesh,
        in_specs=placed,
        out_specs=(
            P("owner", None, "rows"),
            P("owner", None, "rows"),
            P("owner", "rows"),
            P("owner", "rows"),
            P(),
        ),
        check_vma=False,
    )
```

```python
import functools

import jax
import jax.numpy as jnp
from jax import lax
from jax.experimental import pallas as pl
from jax.experimental.pallas import tpu as pltpu
from jax.sharding import PartitionSpec as P

MESH = pl.DeviceIdType.MESH
WINDOW = 2
LOADS = 3
OPENING = 4
LEAD = 4
X_LAG, Y_LAG, HALF_LAG = 1, 2, 3
HELD = LOADS + LEAD
SUMS = 2 * LEAD + 2
WRITES = 4


def peer_steps(n):
    far = list(range(2, n, 2))
    return far + [k + 1 for k in far] + [1]


def toggled(index, k):
    result, bit = index, 1
    while bit <= k:
        if k & bit:
            result = result + bit * (1 - 2 * lax.rem(index // bit, 2))
        bit *= 2
    return result


def exchange(
    experts, n, owners, depth, steps,
    gate, up, router, gain,
    pieces, routed, scales,
    window, stage, weight, gains, part, early, partner, chip, others, whole,
    load_sem, first_sem, send_sem, recv_sem, pair_send, pair_recv, sum_send, sum_recv, last_send, last_recv,
    early_send, early_recv, in_sem, r_send, r_recv, z_send, z_recv, c_send, c_recv,
):
    me, mine = lax.axis_index("rows"), lax.axis_index("owner")
    units, piece, rows, width = 2 * experts, pieces.shape[1], gate.shape[1], gate.shape[2]
    lead = early.shape[1]
    peers = [toggled(me, k) for k in peer_steps(n)]
    alike = [toggled(me, k) for k in range(2, n, 2)]
    core, beside = lax.rem(me, 2), toggled(me, 1)
    below, above = lax.max(mine - 1, 0), lax.min(mine + 1, owners - 1)

    barrier = pltpu.get_barrier_semaphore()
    for p in peers:
        pl.semaphore_signal(barrier, inc=1, device_id=(mine, p), device_id_type=MESH)

    @pl.when(mine < owners - 1)
    def _():
        pl.semaphore_signal(barrier, inc=1, device_id=(above, me), device_id_type=MESH)

    def load(s, go):
        for matrix, first in ((gate, 0), (up, experts)):
            @pl.when((s >= first) & (s < first + experts))
            def _():
                slot = lax.rem(s, HELD)
                copy = pltpu.make_async_copy(matrix.at[s - first], window.at[slot], load_sem.at[slot])
                copy.start() if go else copy.wait()

    def pair(s):
        slot = lax.rem(s, SUMS)
        return pltpu.make_async_remote_copy(
            part.at[s, 1 - core], partner.at[s], pair_send.at[slot], pair_recv.at[slot],
            device_id=(mine, beside), device_id_type=MESH,
        )

    def chips(s, t):
        slot = lax.rem(s, SUMS)
        return pltpu.make_async_remote_copy(
            chip.at[s, t], others.at[s, t], sum_send.at[slot, t], sum_recv.at[slot, t],
            device_id=(mine, toggled(me, steps[t])), device_id_type=MESH,
        )

    def halves(s):
        slot = lax.rem(s, SUMS)
        return pltpu.make_async_remote_copy(
            whole.at[s, core], whole.at[s, core], last_send.at[slot], last_recv.at[slot],
            device_id=(mine, beside), device_id_type=MESH,
        )

    def direct(g):
        first, count = ((0, 1), (1, lead - 1))[g]
        return [
            pltpu.make_async_remote_copy(
                part.at[pl.ds(first, count)], early.at[me, pl.ds(first, count)],
                early_send.at[g, i], early_recv.at[g, i],
                device_id=(mine, p), device_id_type=MESH,
            )
            for i, p in enumerate(peers)
        ]

    def far(s):
        slot, land = lax.rem(s, WINDOW), lax.rem(s, 2 * WINDOW)
        return [
            pltpu.make_async_remote_copy(
                stage.at[slot, pl.ds(pl.multiple_of(p * piece, piece), piece)],
                pieces.at[s, :, pl.ds(pl.multiple_of(me * rows, rows), rows)],
                send_sem.at[slot, i], recv_sem.at[land, i],
                device_id=(mine, p), device_id_type=MESH,
            )
            for i, p in enumerate(peers)
        ]

    def start(copies):
        for copy in copies:
            copy.start()

    def finish(copies):
        for copy in copies:
            copy.wait()

    def summed(s):
        half = width // 2
        for h in range(2):
            w = window[lax.rem(s, HELD), :, h * half : (h + 1) * half]
            part[s, h] = jnp.sum(jnp.abs(w), axis=0, keepdims=True)

    def early_total(first, last):
        for h in range(2):
            total = jnp.zeros((last - first, 1, width // 2), jnp.float32)
            for p in range(n):
                total = total + jnp.where(p == me, part[first:last, h], early[p, first:last, h])
            whole[first:last, h] = total

    def scaled(s):
        slot, held = lax.rem(s, WINDOW), lax.rem(s, HELD)
        scale = jnp.concatenate([whole[s, 0], whole[s, 1]], axis=1) / depth
        scales[s] = scale
        inverse = 1.0 / scale
        for at in range(0, width, 128):
            w = window[held, :, at : at + 128] * inverse[:, at : at + 128]
            stage[slot, at : at + 128, :] = w.T.astype(jnp.bfloat16)
        own = stage[slot, pl.ds(pl.multiple_of(me * piece, piece), piece), :]
        pieces[s, :, pl.ds(pl.multiple_of(me * rows, rows), rows)] = own

    fetch = [
        pltpu.make_async_copy(router, weight, in_sem.at[0]),
        pltpu.make_async_copy(gain, gains, in_sem.at[1]),
    ]
    along_rows = [
        pltpu.make_async_remote_copy(
            routed.at[me, mine], routed.at[me, mine], r_send.at[i], r_recv.at[i],
            device_id=(mine, p), device_id_type=MESH,
        )
        for i, p in enumerate(alike)
    ]
    mates = [me] + alike

    def relay(up, step):
        block, side = (mine - step, 1) if up else (mine + step, 0)
        block = lax.max(lax.min(block, owners - 1), 0)
        return [
            pltpu.make_async_remote_copy(
                routed.at[p, block], routed.at[p, block],
                z_send.at[side, step, i], z_recv.at[side, step, i],
                device_id=(above if up else below, me), device_id_type=MESH,
            )
            for i, p in enumerate(mates)
        ]

    def arrival(up, step):
        block, side = (mine - 1 - step, 1) if up else (mine + 1 + step, 0)
        block = lax.max(lax.min(block, owners - 1), 0)
        return [
            pltpu.make_async_remote_copy(
                routed.at[p, block], routed.at[p, block],
                z_send.at[side, step, i], z_recv.at[side, step, i],
                device_id=(above if up else below, me), device_id_type=MESH,
            )
            for i, p in enumerate(mates)
        ]

    def relays(turn):
        for up, step in ((False, turn - 1), (True, turn - 2)):
            if 0 <= step < owners - 1:
                came = (mine > step) if up else (mine + step < owners - 1)
                went = (mine < owners - 1) & (mine >= step) if up else (mine > 0) & (mine + step <= owners - 1)

                @pl.when(came)
                def _():
                    for copy in arrival(up, step):
                        copy.wait_recv()

                @pl.when(went)
                def _():
                    for copy in relay(up, step):
                        copy.wait_send()
        for up, step in ((False, turn), (True, turn - 1)):
            if 0 <= step < owners - 1:
                went = (mine < owners - 1) & (mine >= step) if up else (mine > 0) & (mine + step <= owners - 1)

                @pl.when(went)
                def _():
                    start(relay(up, step))

    across_chip = [
        pltpu.make_async_remote_copy(
            routed.at[p], routed.at[p], c_send.at[i], c_recv.at[i],
            device_id=(mine, beside), device_id_type=MESH,
        )
        for i, p in enumerate(mates)
    ]

    cut = gate.shape[1] // OPENING
    opening = [
        pltpu.make_async_copy(
            gate.at[0, pl.ds(k * cut, cut)], window.at[0, pl.ds(k * cut, cut)], first_sem.at[k]
        )
        for k in range(OPENING)
    ]
    start(opening)
    start(fetch)
    finish(opening)
    summed(jnp.int32(0))
    pl.semaphore_wait(barrier, len(peers) + jnp.where(mine > 0, 1, 0))
    start(direct(0)[::-1])

    @pl.loop(1, HELD)
    def _(s):
        load(s, True)

    finish(fetch)
    routed[me, mine] = (weight[...] * gains[...]).astype(jnp.bfloat16)

    @pl.loop(1, lead)
    def _(s):
        load(s, False)
        summed(s)

    start(direct(1))
    start(along_rows)

    @pl.loop(0, units)
    def _(i):
        def within(s):
            return (s >= lead) & (s < units)

        @pl.when(i >= WINDOW)
        def _():
            finish(far(i - WINDOW))

        @pl.when(i == 0)
        def _():
            finish(direct(0))
            early_total(0, 1)

        @pl.when(i == 1)
        def _():
            finish(direct(1))
            early_total(1, lead)

        @pl.when(i >= lead)
        def _():
            halves(i).wait()

        scaled(i)
        ahead = i + lead

        @pl.when(ahead < units)
        def _():
            load(ahead, False)
            summed(ahead)

        @pl.when(within(ahead - X_LAG))
        def _():
            s = ahead - X_LAG
            pair(s).wait()
            chip[s, 0] = part[s, core] + partner[s]

        @pl.when(within(ahead - Y_LAG))
        def _():
            s = ahead - Y_LAG
            chips(s, 0).wait()
            chip[s, 1] = chip[s, 0] + others[s, 0]

        @pl.when(within(ahead - HALF_LAG))
        def _():
            s = ahead - HALF_LAG
            chips(s, 1).wait()
            whole[s, core] = chip[s, 1] + others[s, 1]

        @pl.when(ahead < units)
        def _():
            pair(ahead).start()

        @pl.when(within(ahead - X_LAG))
        def _():
            chips(ahead - X_LAG, 0).start()

        @pl.when(within(ahead - Y_LAG))
        def _():
            chips(ahead - Y_LAG, 1).start()

        @pl.when(within(ahead - HALF_LAG))
        def _():
            halves(ahead - HALF_LAG).start()

        start(far(i))
        load(ahead + LOADS, True)

        @pl.when(i == LEAD)
        def _():
            finish(along_rows)

        for turn in range(owners + 1):
            @pl.when(i == LEAD + 1 + 2 * turn)
            def _():
                relays(turn)

        @pl.when(i == units // 2)
        def _():
            start(across_chip)

        @pl.when(i == units - units // 4)
        def _():
            finish(across_chip)

    @pl.loop(max(units - WINDOW, 0), units)
    def _(s):
        finish(far(s))


def write_out(
    n, pieces, routed, scales, gate_out, up_out, gate_scale, up_scale, router_out,
    own, table, sems, small,
):
    experts, piece, rest = gate_out.shape[0], gate_out.shape[1], routed.shape[3]
    group = experts // WRITES
    big = [
        pltpu.make_async_copy(
            pieces.at[pl.ds(first + g * group, group)], target.at[pl.ds(g * group, group)],
            sems.at[first // experts, g],
        )
        for target, first in ((gate_out, 0), (up_out, experts))
        for g in range(WRITES)
    ]
    for copy in big:
        copy.start()
    me = lax.axis_index("rows")
    for p in range(n):
        block = routed[p].astype(jnp.float32).reshape(-1, rest)
        table[p * rest : (p + 1) * rest, :] = block.T.astype(jnp.bfloat16)

        @pl.when(me == p)
        def _():
            own[...] = scales[:, 0, p * piece : (p + 1) * piece]

    little = [
        pltpu.make_async_copy(table, router_out, small.at[0]),
        pltpu.make_async_copy(own.at[pl.ds(0, experts)], gate_scale, small.at[1]),
        pltpu.make_async_copy(own.at[pl.ds(experts, experts)], up_scale, small.at[2]),
    ]
    for copy in little:
        copy.start()
    for copy in little + big:
        copy.wait()


def in_kernels(n, owners, w_gate, w_up, router_weight, router_gain):
    experts, rows, width = w_gate.shape
    piece, units, across = width // n, 2 * experts, router_weight.shape[1]
    depth = n * rows
    steps = [1 << b for b in range(1, n.bit_length() - 1)]
    half = width // 2
    anywhere, vmem = pl.BlockSpec(memory_space=pl.ANY), pl.BlockSpec(memory_space=pltpu.VMEM)
    hbm, dma = pl.BlockSpec(memory_space=pltpu.HBM), pltpu.SemaphoreType.DMA
    pieces, routed, scales = pl.pallas_call(
        functools.partial(exchange, experts, n, owners, float(depth), steps),
        out_shape=(
            pltpu.VMEM((units, piece, depth), jnp.bfloat16),
            pltpu.VMEM((n, owners, across, rows), jnp.bfloat16),
            pltpu.VMEM((units, 1, width), jnp.float32),
        ),
        in_specs=[anywhere, anywhere, hbm, hbm],
        out_specs=(vmem, vmem, vmem),
        scratch_shapes=[
            pltpu.VMEM((HELD, rows, width), jnp.float32),
            pltpu.VMEM((WINDOW, width, rows), jnp.bfloat16),
            pltpu.VMEM((across, rows), jnp.float32),
            pltpu.VMEM((1, rows), jnp.float32),
            pltpu.VMEM((units, 2, 1, half), jnp.float32),
            pltpu.VMEM((n, LEAD, 2, 1, half), jnp.float32),
            pltpu.VMEM((units, 1, half), jnp.float32),
            pltpu.VMEM((units, 2, 1, half), jnp.float32),
            pltpu.VMEM((units, 2, 1, half), jnp.float32),
            pltpu.VMEM((units, 2, 1, half), jnp.float32),
            dma((HELD,)), dma((OPENING,)), dma((WINDOW, n - 1)), dma((2 * WINDOW, n - 1)),
            dma((SUMS,)), dma((SUMS,)), dma((SUMS, 2)), dma((SUMS, 2)), dma((SUMS,)), dma((SUMS,)),
            dma((2, n - 1)), dma((2, n - 1)), dma((2,)),
            dma((n // 2,)), dma((n // 2,)), dma((2, owners, n // 2)), dma((2, owners, n // 2)),
            dma((n // 2,)), dma((n // 2,)),
        ],
        compiler_params=pltpu.CompilerParams(
            collective_id=0, has_side_effects=True, vmem_limit_bytes=12 * 2**20
        ),
        name="exchange",
    )(w_gate, w_up, *(pltpu.with_memory_space_constraint(x, pltpu.HBM) for x in (router_weight.T, router_gain[None, :])))

    gate, up, gate_scale, up_scale, router = pl.pallas_call(
        functools.partial(write_out, n),
        out_shape=(
            jax.ShapeDtypeStruct((experts, piece, depth), jnp.bfloat16),
            jax.ShapeDtypeStruct((experts, piece, depth), jnp.bfloat16),
            jax.ShapeDtypeStruct((experts, piece), jnp.float32),
            jax.ShapeDtypeStruct((experts, piece), jnp.float32),
            jax.ShapeDtypeStruct((depth, owners * across), jnp.bfloat16),
        ),
        in_specs=[vmem, vmem, vmem],
        out_specs=(anywhere,) * 5,
        scratch_shapes=[
            pltpu.VMEM((units, piece), jnp.float32),
            pltpu.VMEM((depth, owners * across), jnp.bfloat16),
            dma((2, WRITES)), dma((3,)),
        ],
        compiler_params=pltpu.CompilerParams(vmem_limit_bytes=1 * 2**20),
        name="write_out",
    )(*(pltpu.with_memory_space_constraint(x, pltpu.VMEM) for x in (pieces, routed, scales)))
    return jnp.swapaxes(gate, 1, 2), jnp.swapaxes(up, 1, 2), gate_scale, up_scale, router


def in_ops(n, w_gate, w_up, router_weight, router_gain):
    depth = n * w_gate.shape[1]
    sums = (jnp.sum(jnp.abs(w_gate), axis=1), jnp.sum(jnp.abs(w_up), axis=1))
    served, scales = [], []
    for w, total in zip((w_gate, w_up), lax.psum(sums, "rows")):
        scale = total / depth
        narrow = (w / jnp.expand_dims(scale, 1)).astype(jnp.bfloat16)
        piece = lax.all_to_all(narrow, "rows", split_axis=2, concat_axis=1, tiled=True)
        size = piece.shape[2]
        served.append(piece)
        scales.append(lax.dynamic_slice_in_dim(scale, lax.axis_index("rows") * size, size, axis=1))
    part = (router_weight * router_gain[:, None]).astype(jnp.bfloat16)
    router = lax.all_gather(part, "rows", axis=0, tiled=True)
    router = lax.all_gather(router, "owner", axis=1, tiled=True)
    return (*served, *scales, router)


def solution(mesh):
    n, owners = mesh.shape["rows"], mesh.shape["owner"]

    def on_device(w_gate, w_up, router_weight, router_gain):
        experts, rows, width = w_gate.shape
        whole_tiles = (
            rows % 128 == 0 and width % (16 * n) == 0 and width % 256 == 0
            and n == 8 and owners > 1 and experts % WRITES == 0 and experts >= LEAD + 3 + 2 * owners
        )
        if whole_tiles:
            return in_kernels(n, owners, w_gate, w_up, router_weight, router_gain)
        return in_ops(n, w_gate, w_up, router_weight, router_gain)

    placed = (P("owner", "rows", None), P("owner", "rows", None), P("rows", "owner"), P("rows"))
    return jax.shard_map(
        on_device,
        mesh=mesh,
        in_specs=placed,
        out_specs=(
            P("owner", None, "rows"),
            P("owner", None, "rows"),
            P("owner", "rows"),
            P("owner", "rows"),
            P(),
        ),
        check_vma=False,
    )
```
